8 devices in a mesh: depth: 2 (over z, y), col: 2 (over x), row: 2 (over core).
Axes of the slice: x: 2, y: 2, z: 1, core: 2. Of those that a mesh axis runs over, the one named last changes fastest.
Arguments:
- x: bfloat16 [32, 512, 4096], P(('depth', 'row'), None, 'col')
- ln_scale: float32 [4096], P('col')
- ln_bias: float32 [4096], P('col')
- w_qkv: bfloat16 [4096, 12288], P('row', 'col')
- b_qkv: float32 [32, 384], P('col')
- w_out: bfloat16 [4096, 4096], P('row', 'col')
- b_out: float32 [4096], P('col')
- grad_y: bfloat16 [32, 512, 4096], P(('depth', 'row'), None, 'col')
Outputs:
- output 1: bfloat16 [32, 512, 4096], P(('depth', 'row'), None, 'col')
- output 2: bfloat16 [32, 512, 4096], P(('depth', 'row'), None, 'col')
- output 3: float32 [4096, 12288], P('row', 'col')
- output 4: float32 [32, 384], P('col')
- output 5: float32 [4096, 4096], P('row', 'col')
- output 6: float32 [4096], P('col')
- output 7: float32 [4096], P('col')
- output 8: float32 [4096], P('col')
All inputs are finite; a program needn't handle non-finite values.
Results may differ from the reference program's by a relative error of at most 0.00731328.
Values are sent between devices in bfloat16 or wider.
A program may use at most 1 GiB of HBM per device.

```python
import jax
import jax.numpy as jnp
from jax import lax

TOTAL_BATCH = 32
SEQ_LEN = 512
D_MODEL = 4096
N_HEADS = 32
HEAD_DIM = D_MODEL // N_HEADS


def setup_inputs(seed: int = 0) -> dict:
    key_list = jax.random.split(jax.random.key(seed), 8)
    act_shape = (TOTAL_BATCH, SEQ_LEN, D_MODEL)
    x = jax.random.normal(key_list[0], act_shape, jnp.float32).astype(jnp.bfloat16)
    ln_scale = 1.0 + 0.3 * jax.random.normal(key_list[1], (D_MODEL,), jnp.float32)
    ln_bias = 0.5 * jax.random.normal(key_list[2], (D_MODEL,), jnp.float32)
    w_qkv = (jax.random.normal(key_list[3], (D_MODEL, 3 * D_MODEL), jnp.float32) * D_MODEL ** -0.5).astype(jnp.bfloat16)
    b_qkv = 0.5 * jax.random.normal(key_list[4], (N_HEADS, 3 * HEAD_DIM), jnp.float32)
    w_out = (jax.random.normal(key_list[5], (D_MODEL, D_MODEL), jnp.float32) * (2.0 * D_MODEL ** -0.5)).astype(jnp.bfloat16)
    b_out = 0.5 * jax.random.normal(key_list[6], (D_MODEL,), jnp.float32)
    grad_y = jax.random.normal(key_list[7], act_shape, jnp.float32).astype(jnp.bfloat16)
    return dict(x=x, ln_scale=ln_scale, ln_bias=ln_bias, w_qkv=w_qkv, b_qkv=b_qkv, w_out=w_out, b_out=b_out, grad_y=grad_y)


def attend_sequence(pair):
    qkv_one, d_out_one = pair
    attn_scale = HEAD_DIM ** -0.5
    q_heads = qkv_one[:, :, 0].astype(jnp.float32)
    k_heads = qkv_one[:, :, 1].astype(jnp.float32)
    v_heads = qkv_one[:, :, 2].astype(jnp.float32)
    positions = jnp.arange(SEQ_LEN)
    causal = positions[:, None] >= positions[None, :]
    scores = jnp.einsum('qhe,khe->hqk', q_heads, k_heads) * attn_scale
    attn_prob = jax.nn.softmax(jnp.where(causal, scores, -1e30), axis=-1)
    prob_b = attn_prob.astype(jnp.bfloat16).astype(jnp.float32)
    attn_out = jnp.einsum('hqk,khe->qhe', prob_b, v_heads).astype(jnp.bfloat16)
    d_out32 = d_out_one.astype(jnp.float32)
    d_prob = jnp.einsum('qhe,khe->hqk', d_out32, v_heads)
    d_v = jnp.einsum('hqk,qhe->khe', prob_b, d_out32)
    row_dot = jnp.sum(attn_prob * d_prob, axis=-1, keepdims=True)
    d_scores = (attn_prob * (d_prob - row_dot) * attn_scale).astype(jnp.bfloat16).astype(jnp.float32)
    d_q = jnp.einsum('hqk,khe->qhe', d_scores, k_heads)
    d_k = jnp.einsum('hqk,qhe->khe', d_scores, q_heads)
    d_qkv = jnp.stack([d_q, d_k, d_v], axis=2).astype(jnp.bfloat16)
    return attn_out, d_qkv


def reference(x, ln_scale, ln_bias, w_qkv, b_qkv, w_out, b_out, grad_y):
    tokens = TOTAL_BATCH * SEQ_LEN
    x_f32 = x.reshape(tokens, D_MODEL).astype(jnp.float32)
    g_flat = grad_y.reshape(tokens, D_MODEL)
    mean_x = jnp.mean(x_f32, axis=-1, keepdims=True)
    centered = x_f32 - mean_x
    var_x = jnp.mean(centered * centered, axis=-1, keepdims=True)
    inv_std = lax.rsqrt(var_x + 1e-5)
    x_hat = centered * inv_std
    h_flat = (x_hat * ln_scale + ln_bias).astype(jnp.bfloat16)
    qkv = (jnp.dot(h_flat, w_qkv, preferred_element_type=jnp.float32) + b_qkv.reshape(3 * D_MODEL)).astype(jnp.bfloat16)
    d_out = jnp.dot(g_flat, w_out.T, preferred_element_type=jnp.float32).astype(jnp.bfloat16)
    attn_out, d_qkv = lax.map(attend_sequence, (qkv.reshape(TOTAL_BATCH, SEQ_LEN, N_HEADS, 3, HEAD_DIM), d_out.reshape(TOTAL_BATCH, SEQ_LEN, N_HEADS, HEAD_DIM)))
    o_flat = attn_out.reshape(tokens, D_MODEL)
    dqkv_flat = d_qkv.reshape(tokens, 3 * D_MODEL)
    y_out = (x_f32 + jnp.dot(o_flat, w_out, preferred_element_type=jnp.float32) + b_out).astype(jnp.bfloat16)
    d_w_out = jnp.dot(o_flat.T, g_flat, preferred_element_type=jnp.float32)
    d_b_out = jnp.sum(g_flat.astype(jnp.float32), axis=0)
    d_w_qkv = jnp.dot(h_flat.T, dqkv_flat, preferred_element_type=jnp.float32)
    d_b_qkv = jnp.sum(dqkv_flat.astype(jnp.float32), axis=0).reshape(N_HEADS, 3 * HEAD_DIM)
    d_h = jnp.dot(dqkv_flat, w_qkv.T, preferred_element_type=jnp.float32)
    d_ln_scale = jnp.sum(d_h * x_hat, axis=0)
    d_ln_bias = jnp.sum(d_h, axis=0)
    g_hat = d_h * ln_scale
    d_norm = inv_std * (g_hat - jnp.mean(g_hat, axis=-1, keepdims=True) - x_hat * jnp.mean(g_hat * x_hat, axis=-1, keepdims=True))
    d_x = (g_flat.astype(jnp.float32) + d_norm).astype(jnp.bfloat16)
    act_shape = (TOTAL_BATCH, SEQ_LEN, D_MODEL)
    return (y_out.reshape(act_shape), d_x.reshape(act_shape), d_w_qkv, d_b_qkv, d_w_out, d_b_out, d_ln_scale, d_ln_bias)
```

```python
import functools

import jax
import jax.numpy as jnp
from jax import lax
from jax.experimental import pallas as pl
from jax.experimental.pallas import tpu as pltpu
from jax.sharding import PartitionSpec as P


F32 = jnp.float32
BF16 = jnp.bfloat16
NEG = -1e30
LOG2E = 1.4426950408889634
DEP, COL, ROW = "depth", "col", "row"
SWAP = ((0, 1), (1, 0))


def nt(a, b):
    return lax.dot_general(a, b, (((1,), (1,)), ((), ())), preferred_element_type=F32)


def tn(a, b):
    return lax.dot_general(a, b, (((0,), (0,)), ((), ())), preferred_element_type=F32)


def nn(a, b):
    return lax.dot_general(a, b, (((1,), (0,)), ((), ())), preferred_element_type=F32)


def ln_kernel(d_model, flag_ref, xo_ref, xp_ref, so_ref, bo_ref, sp_ref, bp_ref, *refs):
    h_ref, ha_ref, hb_ref, m_ref, r_ref = refs[-5:]
    half = xo_ref.shape[1]
    xo = xo_ref[...].astype(F32)
    xp = xp_ref[...].astype(F32)
    mean = (jnp.sum(xo, -1, keepdims=True) + jnp.sum(xp, -1, keepdims=True)) / d_model
    co = xo - mean
    cp = xp - mean
    var = (jnp.sum(co * co, -1, keepdims=True) + jnp.sum(cp * cp, -1, keepdims=True)) / d_model
    inv = lax.rsqrt(var + 1e-5)
    m_ref[...] = mean
    r_ref[...] = inv
    ho = (co * inv * so_ref[...] + bo_ref[...]).astype(BF16)
    hp = (cp * inv * sp_ref[...] + bp_ref[...]).astype(BF16)
    flag = flag_ref[0]

    @pl.when(flag == 1)
    def _():
        ha_ref[...] = ho
        hb_ref[...] = hp
        h_ref[:, :half] = ho
        h_ref[:, half:] = hp

    @pl.when(flag == 0)
    def _():
        ha_ref[...] = hp
        hb_ref[...] = ho
        h_ref[:, :half] = hp
        h_ref[:, half:] = ho


def layer_norm(flag, x_own, x_oth, vecs, carry, base, total):
    rows, half = x_own.shape
    blk = 256
    b0 = base // blk
    row_spec = pl.BlockSpec((blk, half), lambda i, f: (i, 0))
    vec_spec = pl.BlockSpec((1, half), lambda i, f: (0, 0))
    any_spec = pl.BlockSpec(memory_space=pl.ANY)
    n_carry = 0 if carry is None else 2
    return pl.pallas_call(
        functools.partial(ln_kernel, 2 * half),
        out_shape=(
            jax.ShapeDtypeStruct((rows, 2 * half), BF16),
            jax.ShapeDtypeStruct((total, half), BF16),
            jax.ShapeDtypeStruct((total, half), BF16),
            jax.ShapeDtypeStruct((rows, 1), F32),
            jax.ShapeDtypeStruct((rows, 1), F32),
        ),
        grid_spec=pltpu.PrefetchScalarGridSpec(
            num_scalar_prefetch=1,
            grid=(rows // blk,),
            in_specs=[row_spec, row_spec, vec_spec, vec_spec, vec_spec, vec_spec] + [any_spec] * n_carry,
            out_specs=(
                pl.BlockSpec((blk, 2 * half), lambda i, f: (i, 0)),
                pl.BlockSpec((blk, half), lambda i, f: (b0 + i, 0)),
                pl.BlockSpec((blk, half), lambda i, f: (b0 + i, 0)),
                pl.BlockSpec((blk, 1), lambda i, f: (i, 0)),
                pl.BlockSpec((blk, 1), lambda i, f: (i, 0)),
            ),
        ),
        input_output_aliases={} if carry is None else {7: 1, 8: 2},
        compiler_params=pltpu.CompilerParams(vmem_limit_bytes=48 * 2**20),
        cost_estimate=pl.CostEstimate(flops=rows * half * 2 * 40, bytes_accessed=rows * half * 12, transcendentals=0),
        name="layer_norm",
    )(flag, x_own, x_oth, *vecs, *(() if carry is None else carry))


def attn_fwd_kernel(heads, hd, qkv_ref, *refs):
    oi_ref, oa_ref = refs[-2:]
    seq = qkv_ref.shape[0]
    blk = 256
    scale = hd ** -0.5
    keep = lax.broadcasted_iota(jnp.int32, (blk, blk), 0) >= lax.broadcasted_iota(jnp.int32, (blk, blk), 1)
    for h in range(heads):
        c = h * 3 * hd
        for qb in range(seq // blk):
            q0 = qb * blk
            q = qkv_ref[q0 : q0 + blk, c : c + hd]
            s_d = jnp.where(keep, nt(q, qkv_ref[q0 : q0 + blk, c + hd : c + 2 * hd]), NEG)
            m = jnp.max(s_d, -1, keepdims=True)
            if qb:
                s_u = nt(q, qkv_ref[:q0, c + hd : c + 2 * hd])
                m = jnp.maximum(m, jnp.max(s_u, -1, keepdims=True))
            p_d = jnp.exp2((s_d - m) * (scale * LOG2E))
            den = jnp.sum(p_d, -1, keepdims=True)
            if qb:
                p_u = jnp.exp2((s_u - m) * (scale * LOG2E))
                den = den + jnp.sum(p_u, -1, keepdims=True)
            inv = 1.0 / den
            o = nn((p_d * inv).astype(BF16), qkv_ref[q0 : q0 + blk, c + 2 * hd : c + 3 * hd])
            if qb:
                o = o + nn((p_u * inv).astype(BF16), qkv_ref[:q0, c + 2 * hd : c + 3 * hd])
            o = o.astype(BF16)
            oi_ref[q0 : q0 + blk, h * hd : (h + 1) * hd] = o
            oa_ref[q0 : q0 + blk, h * hd : (h + 1) * hd] = o


def attn_fwd(qkv, hd, carry, base, total, seq):
    rows, width = qkv.shape
    n_heads = width // (3 * hd)
    hb = 4
    s0 = base // seq
    any_spec = pl.BlockSpec(memory_space=pl.ANY)
    n_carry = 0 if carry is None else 1
    n_seq = rows // seq
    return pl.pallas_call(
        functools.partial(attn_fwd_kernel, hb, hd),
        out_shape=(
            jax.ShapeDtypeStruct((rows, width // 3), BF16),
            jax.ShapeDtypeStruct((total, width // 3), BF16),
        ),
        grid=(n_seq, n_heads // hb),
        in_specs=[pl.BlockSpec((seq, 3 * hd * hb), lambda s, h: (s, h))] + [any_spec] * n_carry,
        out_specs=(
            pl.BlockSpec((seq, hd * hb), lambda s, h: (s, h)),
            pl.BlockSpec((seq, hd * hb), lambda s, h: (s0 + s, h)),
        ),
        input_output_aliases={} if carry is None else {1: 1},
        compiler_params=pltpu.CompilerParams(vmem_limit_bytes=48 * 2**20),
        cost_estimate=pl.CostEstimate(
            flops=n_seq * n_heads * 4 * seq * seq * hd * 2, bytes_accessed=rows * width * 4, transcendentals=n_seq * n_heads * seq * seq
        ),
        name="attn_fwd",
    )(qkv, *(() if carry is None else (carry,)))


def attn_bwd_kernel(heads, hd, qkv_ref, do_ref, *refs):
    dqkv_ref, tok_ref, dk_acc, dv_acc = refs[-4:]
    tok_ref[...] = jnp.zeros_like(tok_ref)
    seq = qkv_ref.shape[0]
    blk = 256
    scale = hd ** -0.5
    keep = lax.broadcasted_iota(jnp.int32, (blk, blk), 0) <= lax.broadcasted_iota(jnp.int32, (blk, blk), 1)
    for h in range(heads):
        c = h * 3 * hd
        for qb in reversed(range(seq // blk)):
            q0 = qb * blk
            q = qkv_ref[q0 : q0 + blk, c : c + hd]
            do = do_ref[q0 : q0 + blk, h * hd : (h + 1) * hd]
            spans = [(q0, blk, True)] + ([(0, q0, False)] if qb else [])
            s_list = []
            m = None
            for k0, kn, diag in spans:
                s = nt(qkv_ref[k0 : k0 + kn, c + hd : c + 2 * hd], q)
                if diag:
                    s = jnp.where(keep, s, NEG)
                s_list.append(s)
                mm = jnp.max(s, 0, keepdims=True)
                m = mm if m is None else jnp.maximum(m, mm)
            e_list = [jnp.exp2((s - m) * (scale * LOG2E)) for s in s_list]
            den = functools.reduce(lambda a, b: a + b, [jnp.sum(e, 0, keepdims=True) for e in e_list])
            inv = 1.0 / den
            p_list = [e * inv for e in e_list]
            dp_list = [nt(qkv_ref[k0 : k0 + kn, c + 2 * hd : c + 3 * hd], do) for k0, kn, _ in spans]
            dot = functools.reduce(lambda a, b: a + b, [jnp.sum(p * dp, 0, keepdims=True) for p, dp in zip(p_list, dp_list)])
            dq = None
            for (k0, kn, diag), p, dp in zip(spans, p_list, dp_list):
                ds = (p * (dp - dot) * scale).astype(BF16)
                dv = nn(p.astype(BF16), do)
                dk = nn(ds, q)
                part = tn(qkv_ref[k0 : k0 + kn, c + hd : c + 2 * hd], ds)
                dq = part if dq is None else dq + part
                if q0 + blk < seq:
                    dk = dk + dk_acc[k0 : k0 + kn, :]
                    dv = dv + dv_acc[k0 : k0 + kn, :]
                if diag:
                    dqkv_ref[k0 : k0 + kn, c + hd : c + 2 * hd] = dk.astype(BF16)
                    dqkv_ref[k0 : k0 + kn, c + 2 * hd : c + 3 * hd] = dv.astype(BF16)
                else:
                    dk_acc[k0 : k0 + kn, :] = dk
                    dv_acc[k0 : k0 + kn, :] = dv
            dqkv_ref[q0 : q0 + blk, c : c + hd] = dq.T.astype(BF16)


def attn_bwd(qkv, do, hd, carry, base, total, seq):
    rows, width = qkv.shape
    n_heads = width // (3 * hd)
    hb = 4
    s0 = base // seq
    any_spec = pl.BlockSpec(memory_space=pl.ANY)
    n_carry = 0 if carry is None else 1
    n_seq = rows // seq
    return pl.pallas_call(
        functools.partial(attn_bwd_kernel, hb, hd),
        out_shape=(jax.ShapeDtypeStruct((total, width), BF16), jax.ShapeDtypeStruct((8, 128), F32)),
        grid=(n_seq, n_heads // hb),
        in_specs=[
            pl.BlockSpec((seq, 3 * hd * hb), lambda s, h: (s, h)),
            pl.BlockSpec((seq, hd * hb), lambda s, h: (s, h)),
        ]
        + [any_spec] * n_carry,
        out_specs=(
            pl.BlockSpec((seq, 3 * hd * hb), lambda s, h: (s0 + s, h)),
            pl.BlockSpec((8, 128), lambda s, h: (0, 0)),
        ),
        scratch_shapes=[pltpu.VMEM((seq, hd), F32), pltpu.VMEM((seq, hd), F32)],
        input_output_aliases={} if carry is None else {2: 0},
        compiler_params=pltpu.CompilerParams(vmem_limit_bytes=48 * 2**20),
        cost_estimate=pl.CostEstimate(
            flops=n_seq * n_heads * 10 * seq * seq * hd * 2, bytes_accessed=rows * width * 6, transcendentals=n_seq * n_heads * seq * seq
        ),
        name="attn_bwd",
    )(qkv, do, *(() if carry is None else (carry,)))


class Line:
    def __init__(self):
        self.last = None

    def __call__(self, *vals):
        if self.last is None:
            return vals
        return lax.optimization_barrier(tuple(vals) + (self.last,))[:-1]

    def mark(self, v):
        self.last = v


def solution(mesh):
    act_spec = P((DEP, ROW), None, COL)
    vec_spec = P(COL)
    mat_spec = P(ROW, COL)
    head_vec_spec = P(COL, None)

    def block_fn(x, ln_scale, ln_bias, w_qkv, b_qkv, w_out, b_out, grad_y):
        n_seq, seq, dl = x.shape
        tok = n_seq * seq
        d_model = 2 * dl
        heads, three_hd = b_qkv.shape
        hd = three_hd // 3
        wide = heads * three_hd
        depth = lax.axis_index(DEP)
        col = lax.axis_index(COL)
        row = lax.axis_index(ROW)
        same = row == col
        X = x.reshape(tok, dl)
        G = grad_y.reshape(tok, dl)

        sizes = [2, 2, 2, 1, 1] if n_seq == 8 else [1] * n_seq
        spans = []
        at = 0
        for n in sizes:
            spans.append((at * seq, n * seq))
            at += n
        nc = len(spans)
        line = Line()

        def over(axis, v):
            return lax.ppermute(v, axis, SWAP)

        vec_oth = over(COL, jnp.concatenate([ln_scale, ln_bias]))
        vecs = (ln_scale.reshape(1, dl), ln_bias.reshape(1, dl), vec_oth[:dl].reshape(1, dl), vec_oth[dl:].reshape(1, dl))
        xs = [lax.slice_in_dim(X, a, a + n, axis=0) for a, n in spans]
        xr = [over(COL, xs[i]) for i in range(nc)]
        gs = [lax.slice_in_dim(G, a, a + n, axis=0) for a, n in spans]
        gr = {}

        w_peer = over(ROW, w_qkv)
        wo_peer = over(ROW, w_out)
        wo_own = jnp.where(same, w_out, wo_peer)
        wo_oth = jnp.where(same, wo_peer, w_out)
        line.mark(wo_oth)
        quarter = dl // 4
        qi = 2 * depth + row
        qt = over(COL, lax.dynamic_slice_in_dim(wo_oth, qi * quarter, quarter, axis=0))
        (wqa, wqb) = line(w_qkv, w_peer)
        w_cat = jnp.concatenate([wqa, wqb], axis=0)
        line.mark(w_cat)

        flag = same.astype(jnp.int32).reshape(1)
        bq = b_qkv.reshape(1, wide)
        hc, o_all = None, None
        qkvs, outs, means, invs = [], [], [], []
        g_after = {0: (0, 1), 1: (2,), 2: (3, 4)}
        for i, (a, n) in enumerate(spans):
            (xi, xri) = line(xs[i], xr[i])
            h, ha, hb, mean, inv = layer_norm(flag, xi, xri, vecs, hc, a, tok)
            hc = (ha, hb)
            means.append(mean)
            invs.append(inv)
            qkv = (nn(h, w_cat) + bq).astype(BF16)
            o, o_all = attn_fwd(qkv, hd, o_all, a, tok, seq)
            line.mark(o)
            qkvs.append(qkv)
            outs.append(o)
            for k in g_after.get(i, ()):
                (gk,) = line(gs[k])
                gr[k] = over(COL, gk)
        h_keep, h_send = hc

        (qt,) = line(qt)
        qt_r = over(ROW, qt)

        jo = (COL, ROW)
        ja = (DEP, COL, ROW)
        (g_e,) = line(G)
        early = tn(o_all, g_e)
        line.mark(early)
        early_p = lax.ppermute(early, jo, ((1, 0), (2, 3)))
        (qt, qt_r) = line(qt, qt_r)
        pair = jnp.where(row == 0, jnp.concatenate([qt, qt_r]), jnp.concatenate([qt_r, qt]))
        pair_d = over(DEP, pair)
        wo_blk = jnp.where(depth == 0, jnp.concatenate([pair, pair_d]), jnp.concatenate([pair_d, pair]))
        line.mark(wo_blk)

        dqkv = None
        ors = {}
        o_after = {2: (0, 1), 3: (2,), 4: (3, 4)}
        for i, (a, n) in enumerate(spans):
            (gi, gri) = line(gs[i], gr[i])
            do = (nt(gi, wo_own) + nt(gri, wo_blk)).astype(BF16)
            dqkv, t = attn_bwd(qkvs[i], do, hd, dqkv, a, tok, seq)
            line.mark(t)
            if i == 0:
                (e1, e2) = line(early, early_p)
                early = e1 + e2
                line.mark(early)
                early_y = lax.ppermute(early, ja, ((0, 4), (4, 0), (3, 7), (7, 3)))
            for k in o_after.get(i, ()):
                (ok,) = line(outs[k])
                ors[k] = over(COL, ok)

        n_j = 6
        wj = wide // n_j
        parts, sums, ys = {}, {}, {}
        dh_own, dh_rec = {}, {}

        def send(j):
            (hs, dd) = line(h_send, dqkv)
            v = tn(hs, lax.slice_in_dim(dd, j * wj, (j + 1) * wj, axis=1))
            line.mark(v)
            parts[j] = over(ROW, v)

        def keep(j):
            (hk, dd, pj) = line(h_keep, dqkv, parts[j])
            v = tn(hk, lax.slice_in_dim(dd, j * wj, (j + 1) * wj, axis=1)) + pj
            line.mark(v)
            sums[j] = v
            ys[j] = over(DEP, v)

        def dho(i):
            a, n = spans[i]
            (dd, ww) = line(dqkv, w_oth)
            v = nt(lax.slice_in_dim(dd, a, a + n, axis=0), ww)
            line.mark(v)
            dh_rec[i] = over(COL, v)

        def dhk(i):
            a, n = spans[i]
            (dd, ww) = line(dqkv, w_own)
            v = nt(lax.slice_in_dim(dd, a, a + n, axis=0), ww)
            line.mark(v)
            dh_own[i] = v

        d_w_qkv = None

        def fin(j):
            nonlocal d_w_qkv
            if d_w_qkv is None:
                d_w_qkv = jnp.zeros((dl, wide), F32)
            (s, r) = line(sums[j], ys[j])
            v = s + r
            line.mark(v)
            d_w_qkv = lax.dynamic_update_slice(d_w_qkv, v, (0, j * wj))

        send(0)
        send(1)
        keep(0)
        (wa, wb) = line(w_qkv, w_peer)
        w_own = jnp.where(same, wa, wb)
        w_oth = jnp.where(same, wb, wa)
        line.mark(w_oth)
        send(2)
        keep(1)
        dho(0)
        send(3)
        keep(2)
        dho(1)
        send(4)
        keep(3)
        dho(2)
        send(5)
        keep(4)
        dho(3)
        keep(5)
        dho(4)
        for i in range(nc):
            dhk(i)
        (dd,) = line(dqkv)
        d_b_qkv = jnp.sum(dd.astype(F32), axis=0).reshape(heads, three_hd)
        line.mark(d_b_qkv)
        (gg,) = line(G)
        d_b_out = jnp.sum(gg.astype(F32), axis=0)
        line.mark(d_b_out)

        (o0, o1, o2, o3, o4) = line(*(ors[k] for k in range(nc)))
        o_rec = jnp.concatenate([o0, o1, o2, o3, o4], axis=0)
        (o_rec, gg) = line(o_rec, G)
        late = tn(o_rec, gg)
        line.mark(late)
        late_p = lax.ppermute(late, jo, ((0, 1), (3, 2)))
        (oo, orr) = line(o_all, o_rec)
        y = (X.astype(F32) + nn(oo, wo_own) + nn(orr, wo_oth) + b_out).astype(BF16)
        line.mark(y)
        (l1, l2) = line(late, late_p)
        late = l1 + l2
        line.mark(late)
        late_y = lax.ppermute(late, ja, ((1, 5), (5, 1), (2, 6), (6, 2)))

        d_scale, d_bias, sts, dxs = [], [], [], []

        def dxa(i):
            (own, rec) = line(dh_own[i], dh_rec[i])
            dh = own + rec
            xh = (xs[i].astype(F32) - means[i]) * invs[i]
            g = dh * ln_scale
            d_scale.append(jnp.sum(dh * xh, axis=0))
            d_bias.append(jnp.sum(dh, axis=0))
            st = jnp.stack([jnp.sum(g, axis=-1), jnp.sum(g * xh, axis=-1)])
            line.mark(st)
            sts.append(st)

        def dxb(i):
            a, n = spans[i]
            (own, rec) = line(dh_own[i], dh_rec[i])
            s0 = st_all[0, a : a + n][:, None]
            s1 = st_all[1, a : a + n][:, None]
            xh = (xs[i].astype(F32) - means[i]) * invs[i]
            v = (gs[i].astype(F32) + invs[i] * ((own + rec) * ln_scale - s0 - xh * s1)).astype(BF16)
            line.mark(v)
            dxs.append(v)

        fin(0)
        fin(1)
        dxa(0)
        fin(2)
        dxa(1)
        (e, l, ey, ly) = line(early, late, early_y, late_y)
        d_w_out = jnp.where(same, e + ey, l + ly)
        line.mark(d_w_out)
        dxa(2)
        dxa(3)
        fin(3)
        dxa(4)
        st_all = jnp.concatenate(sts, axis=1)
        st_all = (st_all + over(COL, st_all)) / d_model
        for i in range(nc):
            dxb(i)
        dx = jnp.concatenate(dxs, axis=0)
        d_scale = functools.reduce(lambda p, q: p + q, d_scale)
        d_bias = functools.reduce(lambda p, q: p + q, d_bias)
        (d_b_qkv, d_b_out, d_scale, d_bias) = line(d_b_qkv, d_b_out, d_scale, d_bias)
        d_b_qkv, d_b_out, d_scale, d_bias = lax.psum((d_b_qkv, d_b_out, d_scale, d_bias), (DEP, ROW))
        line.mark(d_bias)
        fin(4)
        fin(5)
        return (y.reshape(x.shape), dx.reshape(x.shape), d_w_qkv, d_b_qkv, d_w_out, d_b_out, d_scale, d_bias)

    return jax.shard_map(
        block_fn,
        mesh=mesh,
        in_specs=(act_spec, vec_spec, vec_spec, mat_spec, head_vec_spec, mat_spec, vec_spec, act_spec),
        out_specs=(act_spec, act_spec, mat_spec, head_vec_spec, mat_spec, vec_spec, vec_spec, vec_spec),
        check_vma=False,
    )
```
